512 devices in a mesh: dp: 64 (over x, z, core), mp: 8 (over y).
Axes of the slice: x: 4, y: 8, z: 8, core: 2. Of those that a mesh axis runs over, the one named last changes fastest.
Arguments:
- inputs: bfloat16 [32768, 3968], P('dp', 'mp'), may hold values from -6 to 6
- grad_out: bfloat16 [32768, 2048], P('dp', 'mp'), may hold values from -0.25 to 0.25
- error: bfloat16 [131072, 3968], P(('dp', 'mp')), may hold values from -6 to 6
- q_prev: float32 [3968, 64], P('mp'), may hold values from -0.09375 to 0.09375
Outputs:
- new_error: bfloat16 [131072, 3968], P(('dp', 'mp'))
- p_basis: float32 [2048, 64], P('mp')
- q_factor: float32 [3968, 64], P('mp')
The draws below stay inside these ranges and needn't reach their ends.
All inputs are finite; a program needn't handle non-finite values.
Results may differ from the reference program's by a relative error of at most 0.0065.
Values may be sent and summed in bfloat16 or wider, within the bound.
No kernel may reach another device: no remote copies, remote signals or barrier semaphores. Data moves between devices by JAX's collectives and lax.ppermute only.
A program may use at most 64 MiB of HBM per device.

```python
import jax
import jax.numpy as jnp
from jax import lax

D = 3968
OUT = 2048
R = 64
TOK_DEV = 512
TOKENS = 32768
ROWS = 131072
N_DP = 64


def block_scale(stream_key, dims, cuts, smallest, top_value):
    level, own = 1.0, jax.random.fold_in(stream_key, 6)
    for dim, parts in cuts:
        steps = jnp.exp(jax.random.uniform(jax.random.fold_in(own, dim), (parts,), jnp.float32, smallest / len(cuts), top_value / len(cuts)))
        level = level * jnp.repeat(steps, dims[dim] // parts).reshape([-1 if axis == dim else 1 for axis in range(len(dims))])
    return level


def noise(rng, shape, scale, limit, split=(), kind=jnp.bfloat16):
    array = jax.random.normal(rng, shape, jnp.float32) * scale
    if len(split) > 0:
        array = block_scale(rng, shape, split, -0.22, 0.18) * array
    return jnp.clip(array, min=-limit, max=limit).astype(kind)


def setup_inputs(seed: int = 0) -> dict:
    arg_keys = jax.random.split(jax.random.key(seed), 5)
    return {
        "inputs": noise(arg_keys[0], (TOKENS, D), 1.0, 6.0, ((0, 64), (1, 8))),
        "grad_out": noise(arg_keys[1], (TOKENS, OUT), TOK_DEV ** -0.5, 0.25, ((0, 64), (1, 8))),
        "error": noise(arg_keys[2], (ROWS, D), 1.0, 6.0, ((0, 512),)),
        "q_prev": noise(arg_keys[3], (D, R), D ** -0.5, 0.09375, ((0, 8),), jnp.float32),
    }


def reference(inputs, grad_out, error, q_prev):
    highest = lax.Precision.HIGHEST
    xs = inputs.reshape(N_DP, TOK_DEV, D)
    gs = grad_out.reshape(N_DP, TOK_DEV, OUT)
    es = error.reshape(N_DP, OUT, D)

    def merged(index):
        xrow = lax.dynamic_index_in_dim(xs, index, 0, False)
        grow = lax.dynamic_index_in_dim(gs, index, 0, False)
        erow = lax.dynamic_index_in_dim(es, index, 0, False)
        prod = lax.dot_general(grow.astype(jnp.float32), xrow.astype(jnp.float32), (((0,), (0,)), ((), ())), preferred_element_type=jnp.float32)
        return prod + erow.astype(jnp.float32)

    def add_p(carry, index):
        return (carry + jnp.dot(merged(index), q_prev, precision=highest), None)
    indices = jnp.arange(N_DP, dtype=jnp.int32)
    psum_all, _ = lax.scan(add_p, jnp.zeros((OUT, R), jnp.float32), indices)
    factor = psum_all / N_DP
    gram = jnp.dot(factor.T, factor, precision=highest)
    ridge = 0.01 * jnp.trace(gram) / R + 1e-06
    gram = gram + ridge * jnp.eye(R, dtype=jnp.float32)
    lower = jnp.linalg.cholesky(gram)
    p_hat = jax.scipy.linalg.solve_triangular(lower, factor.T, lower=True).T

    def add_q(carry, index):
        term = lax.dot_general(merged(index), p_hat, (((0,), (0,)), ((), ())), precision=highest)
        return (carry + term, None)
    qsum_all, _ = lax.scan(add_q, jnp.zeros((D, R), jnp.float32), indices)
    q_factor = qsum_all / N_DP
    approx = jnp.dot(p_hat, q_factor.T, precision=highest)

    def residue(index):
        return (merged(index) - approx).astype(jnp.bfloat16)
    new_error = lax.map(residue, indices).reshape(N_DP * OUT, D)
    return (new_error, p_hat * jnp.sqrt(jnp.float32(OUT)), q_factor)
```

```python
import jax
import jax.numpy as jnp
from jax import lax
from jax.sharding import Mesh
from jax.sharding import PartitionSpec as P

DP = ("dp_0", "dp_1", "dp_2")
DP_MP = ("dp_0", "dp_1", "dp_2", "mp")
BF16 = jnp.bfloat16
F32 = jnp.float32
HIGHEST = lax.Precision.HIGHEST


def exchange(pieces, axes):
    return lax.all_to_all(pieces, axes, split_axis=0, concat_axis=0, tiled=True)


def sent_to_all(shard, axes):
    return exchange(jnp.broadcast_to(shard, (lax.axis_size(axes), *shard.shape)), axes)


def in_columns(blocks):
    return jnp.concatenate([blocks[i] for i in range(blocks.shape[0])], axis=1)


def nt(a, b, **kw):
    return lax.dot_general(a, b, (((1,), (1,)), ((), ())), preferred_element_type=F32, **kw)


def nn(a, b, **kw):
    return lax.dot_general(a, b, (((1,), (0,)), ((), ())), preferred_element_type=F32, **kw)


def two_parts(value):
    high = lax.reduce_precision(value, 8, 7)
    return high.astype(BF16), (value - high).astype(BF16)


def per_device(inputs, grad_out, error, q_prev):
    replicas = lax.axis_size(DP)
    shards = lax.axis_size("mp")
    tokens, cols = inputs.shape
    rows = grad_out.shape[1]
    rank = q_prev.shape[1]
    half = tokens // 2
    x_t = inputs.T
    q_t = q_prev.T

    q_high, q_low = two_parts(q_t)
    xq = nn(q_high, x_t) + nn(q_low, x_t)
    first = sent_to_all(jnp.concatenate([xq.astype(BF16), q_high], axis=1), "mp")
    xq_sum = jnp.sum(first[:, :, :tokens].astype(F32), axis=0)
    q_full = in_columns(first[:, :, tokens:])
    x_a, first_seen = lax.optimization_barrier((inputs[:half], first[0, 0, 0]))
    x_a = lax.all_gather(x_a, "mp", axis=1, tiled=True)

    p_part = nn(xq_sum.astype(BF16), grad_out) + nt(q_full, error)
    p_row = jnp.sum(exchange(p_part, DP), axis=0) / replicas
    p_t = sent_to_all(p_row, DP)

    p_b = p_t.astype(BF16)
    gram_part = nt(p_t, p_t, precision=HIGHEST)
    gram_high, gram_low = two_parts(gram_part)
    gp = nt(p_b, grad_out).astype(BF16)
    ep = nn(p_b, error).astype(BF16)
    same = jnp.concatenate([gp, gram_high, gram_low], axis=1)
    ep_parts = jnp.moveaxis(ep.reshape(rank, shards, cols), 1, 0)
    same_parts = jnp.broadcast_to(same, (shards, *same.shape))
    pieces = jnp.concatenate([same_parts, ep_parts], axis=2)
    second = exchange(pieces, "mp")
    total = jnp.sum(second.astype(F32), axis=0)
    x_b, second_seen = lax.optimization_barrier((inputs[half:], second[0, 0, 0]))
    x_b = lax.all_gather(x_b, "mp", axis=1, tiled=True)
    gp_sum = total[:, :tokens]
    gram = total[:, tokens : tokens + rank] + total[:, tokens + rank : tokens + 2 * rank]
    ep_sum = total[:, tokens + 2 * rank :]

    q_part = nt(gp_sum.astype(BF16), x_t) + ep_sum
    q_row = jnp.sum(exchange(q_part, DP), axis=0) / replicas
    mixed = sent_to_all(q_row, DP)

    ridge = 0.01 * jnp.trace(gram) / rank + 1e-06
    eye = jnp.eye(rank, dtype=F32)
    lower = jnp.linalg.cholesky(gram + ridge * eye, symmetrize_input=False)
    inverse = jax.scipy.linalg.solve_triangular(lower, eye, lower=True)
    p_hat = nn(inverse, p_t, precision=HIGHEST)
    q_own = nn(inverse, mixed, precision=HIGHEST)

    q_whole = in_columns(sent_to_all(q_own.astype(BF16), "mp"))
    tn = (((0,), (0,)), ((), ()))
    merged = (
        lax.dot_general(grad_out[:half], x_a, tn, preferred_element_type=F32)
        + lax.dot_general(grad_out[half:], x_b, tn, preferred_element_type=F32)
        + error.astype(F32)
    )
    approx = lax.dot_general(p_hat.astype(BF16), q_whole, tn, preferred_element_type=F32)
    new_error = (merged - approx).astype(BF16)
    scale = jnp.sqrt(F32(rows * shards))
    return (new_error, (p_hat * scale).T, q_own.T)


def solution(mesh):
    finer = Mesh(mesh.devices.reshape(4, 8, 2, mesh.shape["mp"]), ("dp_0", "dp_1", "dp_2", "mp"))
    in_specs = (P(DP, "mp"), P(DP, "mp"), P(DP_MP, None), P("mp", None))
    out_specs = (P(DP_MP, None), P("mp", None), P("mp", None))
    return jax.shard_map(
        per_device, mesh=finer, in_specs=in_specs, out_specs=out_specs, check_vma=False
    )
```

```python
import jax
import jax.numpy as jnp
from jax import lax
from jax.experimental import pallas as pl
from jax.experimental.pallas import tpu as pltpu
from jax.sharding import Mesh
from jax.sharding import PartitionSpec as P

DP = ("dp_0", "dp_1", "dp_2")
DP_MP = ("dp_0", "dp_1", "dp_2", "mp")
BF16 = jnp.bfloat16
F32 = jnp.float32
HIGHEST = lax.Precision.HIGHEST


def exchange(pieces, axes):
    return lax.all_to_all(pieces, axes, split_axis=0, concat_axis=0, tiled=True)


def sent_to_all(shard, axes):
    return exchange(jnp.broadcast_to(shard, (lax.axis_size(axes), *shard.shape)), axes)


def nt(a, b, **kw):
    return lax.dot_general(a, b, (((1,), (1,)), ((), ())), preferred_element_type=F32, **kw)


def nn(a, b, **kw):
    return lax.dot_general(a, b, (((1,), (0,)), ((), ())), preferred_element_type=F32, **kw)


def local_call(body, name, outs, *args, flops=0):
    spec = pl.BlockSpec(memory_space=pltpu.VMEM)
    moved = sum(a.size * a.dtype.itemsize for a in (*args, *outs))
    return pl.pallas_call(
        body,
        name=name,
        out_shape=list(outs),
        in_specs=[spec] * len(args),
        out_specs=[spec] * len(outs),
        compiler_params=pltpu.CompilerParams(vmem_limit_bytes=16 * 1024 * 1024),
        cost_estimate=pl.CostEstimate(flops=flops, bytes_accessed=moved, transcendentals=0),
    )(*args)


def shaped(shape, dtype):
    return jax.ShapeDtypeStruct(shape, dtype)


def start_body(x_ref, q_ref, out_ref):
    tokens = x_ref.shape[1]
    q = q_ref[...]
    high = q.astype(BF16)
    low = (q - high.astype(F32)).astype(BF16)
    x = x_ref[...]
    out_ref[:, :tokens] = (nn(high, x) + nn(low, x)).astype(BF16)
    out_ref[:, tokens:] = high


def p_body(first_ref, g_ref, e_ref, x_ref, out_ref, x_half_ref):
    tokens = g_ref.shape[0]
    shards = first_ref.shape[0]
    x_half_ref[...] = x_ref[:, : x_half_ref.shape[1]]
    xq = first_ref[0, :, :tokens].astype(F32)
    for i in range(1, shards):
        xq = xq + first_ref[i, :, :tokens].astype(F32)
    q_full = jnp.concatenate([first_ref[i, :, tokens:] for i in range(shards)], axis=1)
    out_ref[...] = nn(xq.astype(BF16), g_ref[...]) + nt(q_full, e_ref[...])


def factors_body(p_ref, g_ref, e_ref, out_ref):
    tokens = g_ref.shape[0]
    shards, rank, width = out_ref.shape
    cols = width - tokens - 2 * rank
    p = p_ref[...]
    p_b = p.astype(BF16)
    gram = nt(p, p, precision=HIGHEST)
    high = gram.astype(BF16)
    low = (gram - high.astype(F32)).astype(BF16)
    gp = nt(p_b, g_ref[...]).astype(BF16)
    ep = nn(p_b, e_ref[...]).astype(BF16)
    both = jnp.concatenate([high, low], axis=1)
    for i in range(shards):
        out_ref[i, :, :tokens] = gp
        out_ref[i, :, tokens : tokens + 2 * rank] = both
        out_ref[i, :, tokens + 2 * rank :] = ep[:, i * cols : (i + 1) * cols]


def q_body(second_ref, x_ref, out_ref, gram_ref, x_half_ref):
    tokens = x_ref.shape[1]
    rank = out_ref.shape[0]
    half = x_half_ref.shape[1]
    x_half_ref[...] = x_ref[:, half:]
    total = second_ref[0].astype(F32)
    for i in range(1, second_ref.shape[0]):
        total = total + second_ref[i].astype(F32)
    both = total[:, tokens : tokens + 2 * rank]
    gram_ref[...] = both[:, :rank] + both[:, rank:]
    out_ref[...] = nt(total[:, :tokens].astype(BF16), x_ref[...]) + total[:, tokens + 2 * rank :]


def inverse_body(gram_ref, out_ref):
    rank = gram_ref.shape[0]
    row = lax.broadcasted_iota(jnp.int32, (rank, rank), 0)
    col = lax.broadcasted_iota(jnp.int32, (rank, rank), 1)
    eye = (row == col).astype(F32)
    gram = gram_ref[...]
    trace = jnp.sum(jnp.sum(gram * eye, axis=1, keepdims=True), axis=0, keepdims=True)
    ridge = 0.01 * trace / rank + 1e-06
    work = jnp.concatenate([gram + ridge * eye, eye], axis=1)
    below = lax.broadcasted_iota(jnp.int32, (rank, 2 * rank), 0)
    done = []
    for k in range(0, rank, 2):
        first, second = work[k : k + 1, :], work[k + 1 : k + 2, :]
        left, right = work[:, k : k + 1], work[:, k + 1 : k + 2]
        root = lax.rsqrt(first[:, k : k + 1])
        first, left = first * root, left * root
        cross = first[:, k + 1 : k + 2]
        root = lax.rsqrt(second[:, k + 1 : k + 2] - cross * cross)
        second = (second - cross * first) * root
        right = (right - cross * left) * root
        done.append(first[:, rank:])
        done.append(second[:, rank:])
        if k + 2 < rank:
            rest = below > k + 1
            work = work - (
                jnp.where(rest, left, 0.0) * first + jnp.where(rest, right, 0.0) * second
            )
    out_ref[...] = jnp.concatenate(done, axis=0)


def column_tiles(width, tile=512):
    return [(start, min(start + tile, width)) for start in range(0, width, tile)]


def merged_body(g_ref, e_ref, xa_ref, xb_ref, out_ref):
    half = xa_ref.shape[1]
    for lo, hi in column_tiles(e_ref.shape[1]):
        made = nt(g_ref[:, :half], xa_ref[lo:hi, :]) + nt(g_ref[:, half:], xb_ref[lo:hi, :])
        out_ref[:, lo:hi] = made + e_ref[:, lo:hi].astype(F32)


def residue_body(q_ref, p_ref, merged_ref, out_ref):
    shards = q_ref.shape[0]
    q_full = jnp.concatenate([q_ref[i] for i in range(shards)], axis=1)
    p_rows = p_ref[...]
    for lo, hi in column_tiles(merged_ref.shape[1]):
        approx = nn(p_rows, q_full[:, lo:hi])
        out_ref[:, lo:hi] = (merged_ref[:, lo:hi] - approx).astype(BF16)


def per_device(inputs, grad_out, error, q_prev):
    replicas = lax.axis_size(DP)
    shards = lax.axis_size("mp")
    tokens, cols = inputs.shape
    rows = grad_out.shape[1]
    rank = q_prev.shape[1]
    half = tokens // 2
    width = error.shape[1]
    x_t = inputs.T

    (packed,) = local_call(
        start_body,
        "start",
        [shaped((rank, tokens + cols), BF16)],
        x_t,
        q_prev.T,
        flops=4 * rank * tokens * cols,
    )
    first = lax.all_gather(packed, "mp")
    p_part, x_a = local_call(
        p_body,
        "p_part",
        [shaped((rank, rows), F32), shaped((cols, half), BF16)],
        first,
        grad_out,
        error,
        x_t,
        flops=2 * rank * rows * (tokens + width),
    )
    x_a = lax.all_gather(x_a, "mp", axis=0, tiled=True)
    p_row = jnp.sum(exchange(p_part, DP), axis=0) / replicas
    p_t = sent_to_all(p_row, DP)

    (pieces,) = local_call(
        factors_body,
        "factors",
        [shaped((shards, rank, tokens + 2 * rank + cols), BF16)],
        p_t,
        grad_out,
        error,
        flops=2 * rank * rows * (tokens + width),
    )
    second = exchange(pieces, "mp")
    q_part, gram, x_b = local_call(
        q_body,
        "q_part",
        [shaped((rank, cols), F32), shaped((rank, rank), F32), shaped((cols, half), BF16)],
        second,
        x_t,
        flops=2 * rank * cols * tokens,
    )
    x_b = lax.all_gather(x_b, "mp", axis=0, tiled=True)
    q_row = jnp.sum(exchange(q_part, DP), axis=0) / replicas
    mixed = sent_to_all(q_row, DP)

    (inverse,) = local_call(
        inverse_body, "inverse", [shaped((rank, rank), F32)], gram, flops=4 * rank**3
    )
    p_hat = nn(inverse, p_t, precision=HIGHEST)
    q_own = nn(inverse, mixed, precision=HIGHEST)

    q_parts = sent_to_all(q_own.astype(BF16), "mp")
    (merged,) = local_call(
        merged_body,
        "merged",
        [shaped((rows, width), F32)],
        grad_out.T,
        error,
        x_a,
        x_b,
        flops=2 * rows * width * tokens,
    )
    (new_error,) = local_call(
        residue_body,
        "residue",
        [shaped((rows, width), BF16)],
        q_parts,
        p_hat.astype(BF16).T,
        merged,
        flops=2 * rows * width * rank,
    )
    scale = jnp.sqrt(F32(rows * shards))
    return (new_error, (p_hat * scale).T, q_own.T)


def solution(mesh):
    finer = Mesh(mesh.devices.reshape(4, 8, 2, mesh.shape["mp"]), ("dp_0", "dp_1", "dp_2", "mp"))
    in_specs = (P(DP, "mp"), P(DP, "mp"), P(DP_MP, None), P("mp", None))
    out_specs = (P(DP_MP, None), P("mp", None), P("mp", None))
    return jax.shard_map(
        per_device, mesh=finer, in_specs=in_specs, out_specs=out_specs, check_vma=False
    )
```

```python
import jax
import jax.numpy as jnp
from jax import lax
from jax.experimental import pallas as pl
from jax.experimental.pallas import tpu as pltpu
from jax.sharding import Mesh
from jax.sharding import PartitionSpec as P

DP = ("dp_0", "dp_1", "dp_2")
DP_MP = ("dp_0", "dp_1", "dp_2", "mp")
BF16 = jnp.bfloat16
F32 = jnp.float32
HIGHEST = lax.Precision.HIGHEST


def exchange(pieces, axes):
    return lax.all_to_all(pieces, axes, split_axis=0, concat_axis=0, tiled=True)


def sent_to_all(shard, axes):
    return exchange(jnp.broadcast_to(shard, (lax.axis_size(axes), *shard.shape)), axes)


def nt(a, b, **kw):
    return lax.dot_general(a, b, (((1,), (1,)), ((), ())), preferred_element_type=F32, **kw)


def nn(a, b, **kw):
    return lax.dot_general(a, b, (((1,), (0,)), ((), ())), preferred_element_type=F32, **kw)


def local_call(body, name, outs, *args, flops=0):
    spec = pl.BlockSpec(memory_space=pltpu.VMEM)
    moved = sum(a.size * a.dtype.itemsize for a in (*args, *outs))
    return pl.pallas_call(
        body,
        name=name,
        out_shape=list(outs),
        in_specs=[spec] * len(args),
        out_specs=[spec] * len(outs),
        compiler_params=pltpu.CompilerParams(vmem_limit_bytes=16 * 1024 * 1024),
        cost_estimate=pl.CostEstimate(flops=flops, bytes_accessed=moved, transcendentals=0),
    )(*args)


def shaped(shape, dtype):
    return jax.ShapeDtypeStruct(shape, dtype)


def start_body(x_ref, q_ref, out_ref):
    tokens = x_ref.shape[1]
    q = q_ref[...]
    high = q.astype(BF16)
    low = (q - high.astype(F32)).astype(BF16)
    x = x_ref[...]
    out_ref[:, :tokens] = (nn(high, x) + nn(low, x)).astype(BF16)
    out_ref[:, tokens:] = high


def p_body(first_ref, g_ref, e_ref, out_ref):
    tokens = g_ref.shape[0]
    shards = first_ref.shape[0]
    xq = first_ref[0, :, :tokens].astype(F32)
    for i in range(1, shards):
        xq = xq + first_ref[i, :, :tokens].astype(F32)
    q_full = jnp.concatenate([first_ref[i, :, tokens:] for i in range(shards)], axis=1)
    out_ref[...] = nn(xq.astype(BF16), g_ref[...]) + nt(q_full, e_ref[...])


def column_tiles(width, tile=512):
    return [(start, min(start + tile, width)) for start in range(0, width, tile)]


def merged_body(p_ref, g_ref, e_ref, x_ref, out_ref, merged_ref):
    shards, rank, size = out_ref.shape
    cols = size - 2 * rank
    p = p_ref[...]
    p_b = p.astype(BF16)
    gram = nt(p, p, precision=HIGHEST)
    high = gram.astype(BF16)
    low = (gram - high.astype(F32)).astype(BF16)
    both = jnp.concatenate([high, low], axis=1)
    g = g_ref[...]
    parts = []
    for lo, hi in column_tiles(e_ref.shape[1]):
        merged = (nt(g, x_ref[lo:hi, :]) + e_ref[:, lo:hi].astype(F32)).astype(BF16)
        merged_ref[:, lo:hi] = merged
        parts.append(nn(p_b, merged).astype(BF16))
    q_part = jnp.concatenate(parts, axis=1)
    for i in range(shards):
        out_ref[i, :, : 2 * rank] = both
        out_ref[i, :, 2 * rank :] = q_part[:, i * cols : (i + 1) * cols]


def total_body(second_ref, out_ref, gram_ref):
    rank = out_ref.shape[0]
    total = second_ref[0].astype(F32)
    for i in range(1, second_ref.shape[0]):
        total = total + second_ref[i].astype(F32)
    gram_ref[...] = total[:, :rank] + total[:, rank : 2 * rank]
    out_ref[...] = total[:, 2 * rank :]


def inverse_body(gram_ref, out_ref):
    rank = gram_ref.shape[0]
    row = lax.broadcasted_iota(jnp.int32, (rank, rank), 0)
    col = lax.broadcasted_iota(jnp.int32, (rank, rank), 1)
    eye = (row == col).astype(F32)
    gram = gram_ref[...]
    trace = jnp.sum(jnp.sum(gram * eye, axis=1, keepdims=True), axis=0, keepdims=True)
    ridge = 0.01 * trace / rank + 1e-06
    work = jnp.concatenate([gram + ridge * eye, eye], axis=1)
    below = lax.broadcasted_iota(jnp.int32, (rank, 2 * rank), 0)
    done = []
    for k in range(0, rank, 2):
        first, second = work[k : k + 1, :], work[k + 1 : k + 2, :]
        left, right = work[:, k : k + 1], work[:, k + 1 : k + 2]
        root = lax.rsqrt(first[:, k : k + 1])
        first, left = first * root, left * root
        cross = first[:, k + 1 : k + 2]
        root = lax.rsqrt(second[:, k + 1 : k + 2] - cross * cross)
        second = (second - cross * first) * root
        right = (right - cross * left) * root
        done.append(first[:, rank:])
        done.append(second[:, rank:])
        if k + 2 < rank:
            rest = below > k + 1
            work = work - (
                jnp.where(rest, left, 0.0) * first + jnp.where(rest, right, 0.0) * second
            )
    out_ref[...] = jnp.concatenate(done, axis=0)


def residue_body(q_ref, p_ref, merged_ref, out_ref):
    shards = q_ref.shape[0]
    q_full = jnp.concatenate([q_ref[i] for i in range(shards)], axis=1)
    p_rows = p_ref[...]
    for lo, hi in column_tiles(merged_ref.shape[1]):
        approx = nn(p_rows, q_full[:, lo:hi])
        out_ref[:, lo:hi] = (merged_ref[:, lo:hi].astype(F32) - approx).astype(BF16)


def per_device(inputs, grad_out, error, q_prev):
    replicas = lax.axis_size(DP)
    shards = lax.axis_size("mp")
    tokens, cols = inputs.shape
    rows = grad_out.shape[1]
    rank = q_prev.shape[1]
    width = error.shape[1]
    x_t = inputs.T
    x_full = lax.all_gather(x_t, "mp", axis=0, tiled=True)

    (packed,) = local_call(
        start_body,
        "start",
        [shaped((rank, tokens + cols), BF16)],
        x_t,
        q_prev.T,
        flops=4 * rank * tokens * cols,
    )
    first = lax.all_gather(packed, "mp")
    (p_part,) = local_call(
        p_body,
        "p_part",
        [shaped((rank, rows), F32)],
        first,
        grad_out,
        error,
        flops=2 * rank * rows * (tokens + width),
    )
    p_row = jnp.sum(exchange(p_part, DP), axis=0) / replicas
    p_t = sent_to_all(p_row, DP)

    pieces, merged = local_call(
        merged_body,
        "merged",
        [shaped((shards, rank, 2 * rank + cols), BF16), shaped((rows, width), BF16)],
        p_t,
        grad_out.T,
        error,
        x_full,
        flops=2 * rows * width * (tokens + rank),
    )
    second = exchange(pieces, "mp")
    q_part, gram = local_call(
        total_body, "total", [shaped((rank, cols), F32), shaped((rank, rank), F32)], second
    )
    q_row = jnp.sum(exchange(q_part, DP), axis=0) / replicas
    mixed = sent_to_all(q_row, DP)

    (inverse,) = local_call(
        inverse_body, "inverse", [shaped((rank, rank), F32)], gram, flops=4 * rank**3
    )
    p_hat = nn(inverse, p_t, precision=HIGHEST)
    q_own = nn(inverse, mixed, precision=HIGHEST)

    q_parts = sent_to_all(q_own.astype(BF16), "mp")
    (new_error,) = local_call(
        residue_body,
        "residue",
        [shaped((rows, width), BF16)],
        q_parts,
        p_hat.astype(BF16).T,
        merged,
        flops=2 * rows * width * rank,
    )
    scale = jnp.sqrt(F32(rows * shards))
    return (new_error, (p_hat * scale).T, q_own.T)


def solution(mesh):
    finer = Mesh(mesh.devices.reshape(4, 8, 2, mesh.shape["mp"]), ("dp_0", "dp_1", "dp_2", "mp"))
    in_specs = (P(DP, "mp"), P(DP, "mp"), P(DP_MP, None), P("mp", None))
    out_specs = (P(DP_MP, None), P("mp", None), P("mp", None))
    return jax.shard_map(
        per_device, mesh=finer, in_specs=in_specs, out_specs=out_specs, check_vma=False
    )
```

```python
import jax
import jax.numpy as jnp
from jax import lax
from jax.experimental import pallas as pl
from jax.experimental.pallas import tpu as pltpu
from jax.sharding import Mesh
from jax.sharding import PartitionSpec as P

DP = ("dp_0", "dp_1", "dp_2")
CHIPS = ("dp_0", "dp_1")
CORE = "dp_2"
DP_MP = ("dp_0", "dp_1", "dp_2", "mp")
BF16 = jnp.bfloat16
F32 = jnp.float32
HIGHEST = lax.Precision.HIGHEST
GRANT = 16 * 1024 * 1024
WIDE_GRANT = 60 * 1024 * 1024


def exchange(pieces, axes):
    return lax.all_to_all(pieces, axes, split_axis=0, concat_axis=0, tiled=True)


def sent_to_all(shard, axes):
    return exchange(jnp.broadcast_to(shard, (lax.axis_size(axes), *shard.shape)), axes)


def nt(a, b, **kw):
    return lax.dot_general(a, b, (((1,), (1,)), ((), ())), preferred_element_type=F32, **kw)


def nn(a, b, **kw):
    return lax.dot_general(a, b, (((1,), (0,)), ((), ())), preferred_element_type=F32, **kw)


def local_call(body, outs, *args, flops=0):
    spec = pl.BlockSpec(memory_space=pltpu.VMEM)
    moved = sum(a.size * a.dtype.itemsize for a in (*args, *outs))
    return pl.pallas_call(
        body,
        out_shape=list(outs),
        in_specs=[spec] * len(args),
        out_specs=[spec] * len(outs),
        compiler_params=pltpu.CompilerParams(vmem_limit_bytes=GRANT),
        cost_estimate=pl.CostEstimate(flops=flops, bytes_accessed=moved, transcendentals=0),
    )(*args)


def shaped(shape, dtype):
    return jax.ShapeDtypeStruct(shape, dtype)


def start_body(x_ref, q_ref, out_ref):
    tokens = x_ref.shape[1]
    q = q_ref[...]
    high = q.astype(BF16)
    low = (q - high.astype(F32)).astype(BF16)
    x = x_ref[...]
    out_ref[:, :tokens] = (nn(high, x) + nn(low, x)).astype(BF16)
    out_ref[:, tokens:] = high


def p_body(first_ref, g_ref, e_ref, out_ref):
    tokens = g_ref.shape[0]
    shards = first_ref.shape[0]
    xq = first_ref[0, :, :tokens].astype(F32)
    for i in range(1, shards):
        xq = xq + first_ref[i, :, :tokens].astype(F32)
    q_full = jnp.concatenate([first_ref[i, :, tokens:] for i in range(shards)], axis=1)
    out_ref[...] = nn(xq.astype(BF16), g_ref[...]) + nt(q_full, e_ref[...])


def column_tiles(width, tile=512):
    return [(start, min(start + tile, width)) for start in range(0, width, tile)]


def merged_body(g_ref, e_hbm, x_hbm, out_ref, e_ref, x_ref, sems):
    copies = []
    for i, (lo, hi) in enumerate(column_tiles(out_ref.shape[1])):
        pair = (
            pltpu.make_async_copy(x_hbm.at[lo:hi, :], x_ref.at[lo:hi, :], sems.at[0, i]),
            pltpu.make_async_copy(e_hbm.at[:, lo:hi], e_ref.at[:, lo:hi], sems.at[1, i]),
        )
        for copy in pair:
            copy.start()
        copies.append(pair)
    g = g_ref[...]
    for (lo, hi), pair in zip(column_tiles(out_ref.shape[1]), copies):
        for copy in pair:
            copy.wait()
        made = nt(g, x_ref[lo:hi, :]) + e_ref[:, lo:hi].astype(F32)
        out_ref[:, lo:hi] = made.astype(BF16)


def merge(g_t, error, x_full):
    rows, width = error.shape
    return pl.pallas_call(
        merged_body,
        name="merged",
        out_shape=shaped((rows, width), BF16),
        in_specs=[
            pl.BlockSpec(memory_space=pltpu.VMEM),
            pl.BlockSpec(memory_space=pltpu.HBM),
            pl.BlockSpec(memory_space=pltpu.HBM),
        ],
        out_specs=pl.BlockSpec(memory_space=pltpu.VMEM),
        scratch_shapes=[
            pltpu.VMEM(error.shape, error.dtype),
            pltpu.VMEM(x_full.shape, x_full.dtype),
            pltpu.SemaphoreType.DMA((2, len(column_tiles(width)))),
        ],
        compiler_params=pltpu.CompilerParams(vmem_limit_bytes=WIDE_GRANT),
        cost_estimate=pl.CostEstimate(
            flops=2 * rows * width * g_t.shape[1],
            bytes_accessed=4 * rows * width + 2 * x_full.size,
            transcendentals=0,
        ),
    )(g_t, error, x_full)


def product_body(p_ref, merged_ref, out_ref, gram_ref):
    rank = p_ref.shape[0]
    p = p_ref[...]
    gram = nt(p, p, precision=HIGHEST)
    high = gram.astype(BF16)
    gram_ref[:, :rank] = high
    gram_ref[:, rank:] = (gram - high.astype(F32)).astype(BF16)
    row = lax.broadcasted_iota(jnp.int32, (rank, rank), 0)
    col = lax.broadcasted_iota(jnp.int32, (rank, rank), 1)
    near = rank // 2
    evens_first = jnp.where(row < near, 2 * row, 2 * (row - near) + 1)
    p_b = nn((col == evens_first).astype(BF16), p.astype(BF16)).astype(BF16)
    for lo, hi in column_tiles(merged_ref.shape[1]):
        out_ref[:, lo:hi] = nn(p_b, merged_ref[:, lo:hi]).astype(BF16)


def pack_body(pair_ref, gram_ref, out_ref):
    _, width = gram_ref.shape
    shards, near, size = out_ref.shape
    both = jnp.concatenate([gram_ref[:near, :], gram_ref[near:, :]], axis=1)
    summed = (pair_ref[:near, :].astype(F32) + pair_ref[near:, :].astype(F32)).astype(BF16)
    cols = size - 2 * width
    for i in range(shards):
        out_ref[i, :, : 2 * width] = both
        out_ref[i, :, 2 * width :] = summed[:, i * cols : (i + 1) * cols]


def total_body(second_ref, out_ref, gram_ref):
    near = out_ref.shape[0]
    rank = gram_ref.shape[0]
    total = second_ref[0].astype(F32)
    for i in range(1, second_ref.shape[0]):
        total = total + second_ref[i].astype(F32)
    gram_ref[:near, :] = total[:, :rank] + total[:, rank : 2 * rank]
    gram_ref[near:, :] = total[:, 2 * rank : 3 * rank] + total[:, 3 * rank : 4 * rank]
    out_ref[...] = total[:, 4 * rank :]


def inverse_body(gram_ref, out_ref):
    rank = gram_ref.shape[0]
    row = lax.broadcasted_iota(jnp.int32, (rank, rank), 0)
    col = lax.broadcasted_iota(jnp.int32, (rank, rank), 1)
    eye = (row == col).astype(F32)
    gram = gram_ref[...]
    trace = jnp.sum(jnp.sum(gram * eye, axis=1, keepdims=True), axis=0, keepdims=True)
    ridge = 0.01 * trace / rank + 1e-06
    work = jnp.concatenate([gram + ridge * eye, eye], axis=1)
    below = lax.broadcasted_iota(jnp.int32, (rank, 2 * rank), 0)
    done = []
    for k in range(0, rank, 2):
        first, second = work[k : k + 1, :], work[k + 1 : k + 2, :]
        left, right = work[:, k : k + 1], work[:, k + 1 : k + 2]
        root = lax.rsqrt(first[:, k : k + 1])
        first, left = first * root, left * root
        cross = first[:, k + 1 : k + 2]
        root = lax.rsqrt(second[:, k + 1 : k + 2] - cross * cross)
        second = (second - cross * first) * root
        right = (right - cross * left) * root
        done.append(first[:, rank:])
        done.append(second[:, rank:])
        if k + 2 < rank:
            rest = below > k + 1
            work = work - (
                jnp.where(rest, left, 0.0) * first + jnp.where(rest, right, 0.0) * second
            )
    out_ref[...] = jnp.concatenate(done, axis=0)


def residue_body(q_ref, p_ref, merged_ref, out_hbm, out_ref, sems):
    shards = q_ref.shape[0]
    q_full = jnp.concatenate([q_ref[i] for i in range(shards)], axis=1)
    p_rows = p_ref[...]
    copies = []
    for i, (lo, hi) in enumerate(column_tiles(merged_ref.shape[1])):
        approx = nn(p_rows, q_full[:, lo:hi])
        out_ref[:, lo:hi] = (merged_ref[:, lo:hi].astype(F32) - approx).astype(BF16)
        copies.append(
            pltpu.make_async_copy(out_ref.at[:, lo:hi], out_hbm.at[:, lo:hi], sems.at[i])
        )
        copies[-1].start()
    for copy in copies:
        copy.wait()


def residue(q_parts, p_rows, merged):
    rows, width = merged.shape
    spec = pl.BlockSpec(memory_space=pltpu.VMEM)
    return pl.pallas_call(
        residue_body,
        name="residue",
        out_shape=shaped((rows, width), BF16),
        in_specs=[spec] * 3,
        out_specs=pl.BlockSpec(memory_space=pltpu.HBM),
        scratch_shapes=[
            pltpu.VMEM((rows, width), BF16),
            pltpu.SemaphoreType.DMA((len(column_tiles(width)),)),
        ],
        compiler_params=pltpu.CompilerParams(vmem_limit_bytes=GRANT),
        cost_estimate=pl.CostEstimate(
            flops=2 * rows * width * p_rows.shape[1],
            bytes_accessed=4 * rows * width,
            transcendentals=0,
        ),
    )(q_parts, p_rows, merged)


def layer(inputs, grad_out, error, q_prev):
    replicas = lax.axis_size(DP)
    shards = lax.axis_size("mp")
    tokens, cols = inputs.shape
    rows = grad_out.shape[1]
    rank = q_prev.shape[1]
    width = error.shape[1]
    x_t = inputs.T
    x_full = lax.all_gather(x_t, "mp", axis=0, tiled=True)

    (packed,) = local_call(
        start_body,
        [shaped((rank, tokens + cols), BF16)],
        x_t,
        q_prev.T,
        flops=4 * rank * tokens * cols,
    )
    first = lax.all_gather(packed, "mp")
    (p_part,) = local_call(
        p_body,
        [shaped((rank, rows), F32)],
        first,
        grad_out,
        error,
        flops=2 * rank * rows * (tokens + width),
    )
    p_row = jnp.sum(exchange(p_part, DP), axis=0) / replicas
    p_t = sent_to_all(p_row, DP)

    merged = merge(grad_out.T, error, x_full)
    product, gram_part = local_call(
        product_body,
        [shaped((rank, width), BF16), shaped((rank, 2 * rank), BF16)],
        p_t,
        merged,
        flops=2 * rows * width * rank,
    )
    near = rank // lax.axis_size(CORE)
    (pieces,) = local_call(
        pack_body,
        [shaped((shards, near, 4 * rank + cols), BF16)],
        exchange(product, CORE),
        gram_part,
    )
    q_part, gram = local_call(
        total_body, [shaped((near, cols), F32), shaped((rank, rank), F32)], exchange(pieces, "mp")
    )
    q_row = jnp.sum(exchange(q_part, CHIPS), axis=0) / replicas
    mixed = sent_to_all(q_row, DP)

    (inverse,) = local_call(inverse_body, [shaped((rank, rank), F32)], gram, flops=4 * rank**3)
    p_hat = nn(inverse, p_t, precision=HIGHEST)
    q_own = nn(inverse, mixed, precision=HIGHEST)

    q_parts = sent_to_all(q_own.astype(BF16), "mp")
    new_error = residue(q_parts, p_hat.astype(BF16).T, merged)
    scale = jnp.sqrt(F32(rows * shards))
    return (new_error, (p_hat * scale).T, q_own.T)


def solution(mesh):
    finer = Mesh(mesh.devices.reshape(4, 8, 2, mesh.shape["mp"]), ("dp_0", "dp_1", "dp_2", "mp"))
    in_specs = (P(DP, "mp"), P(DP, "mp"), P(DP_MP, None), P("mp", None))
    out_specs = (P(DP_MP, None), P("mp", None), P("mp", None))
    return jax.shard_map(layer, mesh=finer, in_specs=in_specs, out_specs=out_specs, check_vma=False)
```

```python
import jax
import jax.numpy as jnp
from jax import lax
from jax.experimental import pallas as pl
from jax.experimental.pallas import tpu as pltpu
from jax.sharding import Mesh
from jax.sharding import PartitionSpec as P

DP = ("dp_0", "dp_1", "dp_2")
CHIPS = ("dp_0", "dp_1")
CORE = "dp_2"
DP_MP = ("dp_0", "dp_1", "dp_2", "mp")
BF16 = jnp.bfloat16
F32 = jnp.float32
HIGHEST = lax.Precision.HIGHEST
GRANT = 16 * 1024 * 1024
WIDE_GRANT = 50 * 1024 * 1024


def exchange(pieces, axes):
    return lax.all_to_all(pieces, axes, split_axis=0, concat_axis=0, tiled=True)


def sent_to_all(shard, axes):
    return exchange(jnp.broadcast_to(shard, (lax.axis_size(axes), *shard.shape)), axes)


def nt(a, b, **kw):
    return lax.dot_general(a, b, (((1,), (1,)), ((), ())), preferred_element_type=F32, **kw)


def nn(a, b, **kw):
    return lax.dot_general(a, b, (((1,), (0,)), ((), ())), preferred_element_type=F32, **kw)


def local_call(body, outs, *args, flops=0):
    spec = pl.BlockSpec(memory_space=pltpu.VMEM)
    moved = sum(a.size * a.dtype.itemsize for a in (*args, *outs))
    return pl.pallas_call(
        body,
        out_shape=list(outs),
        in_specs=[spec] * len(args),
        out_specs=[spec] * len(outs),
        compiler_params=pltpu.CompilerParams(vmem_limit_bytes=GRANT),
        cost_estimate=pl.CostEstimate(flops=flops, bytes_accessed=moved, transcendentals=0),
    )(*args)


def shaped(shape, dtype):
    return jax.ShapeDtypeStruct(shape, dtype)


def start_body(x_ref, q_ref, out_ref):
    tokens = x_ref.shape[1]
    q = q_ref[...]
    high = q.astype(BF16)
    low = (q - high.astype(F32)).astype(BF16)
    x = x_ref[...]
    out_ref[:, :tokens] = (nn(high, x) + nn(low, x)).astype(BF16)
    out_ref[:, tokens:] = high


def p_body(first_ref, g_ref, e_ref, out_ref):
    tokens = g_ref.shape[0]
    shards = first_ref.shape[0]
    xq = first_ref[0, :, :tokens].astype(F32)
    for i in range(1, shards):
        xq = xq + first_ref[i, :, :tokens].astype(F32)
    q_full = jnp.concatenate([first_ref[i, :, tokens:] for i in range(shards)], axis=1)
    out_ref[...] = nn(xq.astype(BF16), g_ref[...]) + nt(q_full, e_ref[...])


def column_tiles(width, tile=512):
    return [(start, min(start + tile, width)) for start in range(0, width, tile)]


def merged_body(g_ref, e_hbm, x_hbm, out_ref, e_ref, x_ref, sems):
    copies = []
    for i, (lo, hi) in enumerate(column_tiles(out_ref.shape[1])):
        pair = (
            pltpu.make_async_copy(x_hbm.at[lo:hi, :], x_ref.at[lo:hi, :], sems.at[0, i]),
            pltpu.make_async_copy(e_hbm.at[:, lo:hi], e_ref.at[:, lo:hi], sems.at[1, i]),
        )
        for copy in pair:
            copy.start()
        copies.append(pair)
    g = g_ref[...]
    for (lo, hi), pair in zip(column_tiles(out_ref.shape[1]), copies):
        for copy in pair:
            copy.wait()
        made = nt(g, x_ref[lo:hi, :]) + e_ref[:, lo:hi].astype(F32)
        out_ref[:, lo:hi] = made.astype(BF16)


def merge(g_t, error, x_full):
    rows, width = error.shape
    return pl.pallas_call(
        merged_body,
        name="merged",
        out_shape=shaped((rows, width), BF16),
        in_specs=[
            pl.BlockSpec(memory_space=pltpu.VMEM),
            pl.BlockSpec(memory_space=pltpu.HBM),
            pl.BlockSpec(memory_space=pltpu.HBM),
        ],
        out_specs=pl.BlockSpec(memory_space=pltpu.VMEM),
        scratch_shapes=[
            pltpu.VMEM(error.shape, error.dtype),
            pltpu.VMEM(x_full.shape, x_full.dtype),
            pltpu.SemaphoreType.DMA((2, len(column_tiles(width)))),
        ],
        compiler_params=pltpu.CompilerParams(vmem_limit_bytes=WIDE_GRANT),
        cost_estimate=pl.CostEstimate(
            flops=2 * rows * width * g_t.shape[1],
            bytes_accessed=4 * rows * width + 2 * x_full.size,
            transcendentals=0,
        ),
    )(g_t, error, x_full)


def product_body(p_ref, merged_ref, out_ref, gram_ref):
    rank = p_ref.shape[0]
    p = p_ref[...]
    gram = nt(p, p, precision=HIGHEST)
    high = gram.astype(BF16)
    gram_ref[:, :rank] = high
    gram_ref[:, rank:] = (gram - high.astype(F32)).astype(BF16)
    row = lax.broadcasted_iota(jnp.int32, (rank, rank), 0)
    col = lax.broadcasted_iota(jnp.int32, (rank, rank), 1)
    near = rank // 2
    evens_first = jnp.where(row < near, 2 * row, 2 * (row - near) + 1)
    p_b = nn((col == evens_first).astype(BF16), p.astype(BF16)).astype(BF16)
    for lo, hi in column_tiles(merged_ref.shape[1]):
        out_ref[:, lo:hi] = nn(p_b, merged_ref[:, lo:hi]).astype(BF16)


def pack_body(pair_ref, gram_ref, out_ref):
    _, width = gram_ref.shape
    shards, near, size = out_ref.shape
    both = jnp.concatenate([gram_ref[:near, :], gram_ref[near:, :]], axis=1)
    summed = (pair_ref[:near, :].astype(F32) + pair_ref[near:, :].astype(F32)).astype(BF16)
    cols = size - 2 * width
    for i in range(shards):
        out_ref[i, :, : 2 * width] = both
        out_ref[i, :, 2 * width :] = summed[:, i * cols : (i + 1) * cols]


def total_body(second_ref, out_ref, gram_ref):
    near = out_ref.shape[0]
    rank = gram_ref.shape[0]
    total = second_ref[0].astype(F32)
    for i in range(1, second_ref.shape[0]):
        total = total + second_ref[i].astype(F32)
    gram_ref[:near, :] = total[:, :rank] + total[:, rank : 2 * rank]
    gram_ref[near:, :] = total[:, 2 * rank : 3 * rank] + total[:, 3 * rank : 4 * rank]
    out_ref[...] = total[:, 4 * rank :]


def inverse_body(gram_ref, out_ref):
    rank = gram_ref.shape[0]
    row = lax.broadcasted_iota(jnp.int32, (rank, rank), 0)
    col = lax.broadcasted_iota(jnp.int32, (rank, rank), 1)
    eye = (row == col).astype(F32)
    gram = gram_ref[...]
    trace = jnp.sum(jnp.sum(gram * eye, axis=1, keepdims=True), axis=0, keepdims=True)
    ridge = 0.01 * trace / rank + 1e-06
    work = jnp.concatenate([gram + ridge * eye, eye], axis=1)
    below = lax.broadcasted_iota(jnp.int32, (rank, 2 * rank), 0)
    done = []
    for k in range(0, rank, 2):
        first, second = work[k : k + 1, :], work[k + 1 : k + 2, :]
        pivot = jnp.broadcast_to(first[:, k : k + 1], first.shape)
        cross = jnp.broadcast_to(first[:, k + 1 : k + 2], first.shape)
        pivot_2 = jnp.broadcast_to(second[:, k + 1 : k + 2], first.shape)
        left = jnp.broadcast_to(work[:, k : k + 1], work.shape)
        right = jnp.broadcast_to(work[:, k + 1 : k + 2], work.shape)
        root = lax.rsqrt(pivot)
        cross = cross * root
        root_2 = lax.rsqrt(pivot_2 - cross * cross)
        first = first * root
        second = (second - cross * first) * root_2
        done.append(first[:, rank:])
        done.append(second[:, rank:])
        if k + 2 < rank:
            rest = below > k + 1
            left = left * root
            right = (right - cross * left) * root_2
            change = left * first + right * second
            work = jnp.where(rest, work - change, work)
    out_ref[...] = jnp.concatenate(done, axis=0)


def own_body(inverse_ref, mixed_ref, own_ref, out_ref):
    own = nn(inverse_ref[...], mixed_ref[...], precision=HIGHEST)
    own_ref[...] = own
    rounded = own.astype(BF16)
    for i in range(out_ref.shape[0]):
        out_ref[i] = rounded


def residue_body(q_ref, p_ref, merged_ref, out_hbm, out_ref, sems):
    shards = q_ref.shape[0]
    q_full = jnp.concatenate([q_ref[i] for i in range(shards)], axis=1)
    p_rows = p_ref[...]
    copies = []
    for i, (lo, hi) in enumerate(column_tiles(merged_ref.shape[1])):
        approx = nn(p_rows, q_full[:, lo:hi])
        out_ref[:, lo:hi] = (merged_ref[:, lo:hi].astype(F32) - approx).astype(BF16)
        copies.append(
            pltpu.make_async_copy(out_ref.at[:, lo:hi], out_hbm.at[:, lo:hi], sems.at[i])
        )
        copies[-1].start()
    for copy in copies:
        copy.wait()


def residue(q_parts, p_rows, merged):
    rows, width = merged.shape
    spec = pl.BlockSpec(memory_space=pltpu.VMEM)
    return pl.pallas_call(
        residue_body,
        name="residue",
        out_shape=shaped((rows, width), BF16),
        in_specs=[spec] * 3,
        out_specs=pl.BlockSpec(memory_space=pltpu.HBM),
        scratch_shapes=[
            pltpu.VMEM((rows, width), BF16),
            pltpu.SemaphoreType.DMA((len(column_tiles(width)),)),
        ],
        compiler_params=pltpu.CompilerParams(vmem_limit_bytes=GRANT),
        cost_estimate=pl.CostEstimate(
            flops=2 * rows * width * p_rows.shape[1],
            bytes_accessed=4 * rows * width,
            transcendentals=0,
        ),
    )(q_parts, p_rows, merged)


def layer(inputs, grad_out, error, q_prev):
    replicas = lax.axis_size(DP)
    shards = lax.axis_size("mp")
    tokens, cols = inputs.shape
    rows = grad_out.shape[1]
    rank = q_prev.shape[1]
    width = error.shape[1]
    x_t = inputs.T
    x_full = lax.all_gather(x_t, "mp", axis=0, tiled=True)

    (packed,) = local_call(
        start_body,
        [shaped((rank, tokens + cols), BF16)],
        x_t,
        q_prev.T,
        flops=4 * rank * tokens * cols,
    )
    first = lax.all_gather(packed, "mp")
    (p_part,) = local_call(
        p_body,
        [shaped((rank, rows), F32)],
        first,
        grad_out,
        error,
        flops=2 * rank * rows * (tokens + width),
    )
    p_row = jnp.sum(exchange(p_part, DP), axis=0) / replicas
    p_t = sent_to_all(p_row, DP)

    merged = merge(grad_out.T, error, x_full)
    product, gram_part = local_call(
        product_body,
        [shaped((rank, width), BF16), shaped((rank, 2 * rank), BF16)],
        p_t,
        merged,
        flops=2 * rows * width * rank,
    )
    near = rank // lax.axis_size(CORE)
    (pieces,) = local_call(
        pack_body,
        [shaped((shards, near, 4 * rank + cols), BF16)],
        exchange(product, CORE),
        gram_part,
    )
    q_part, gram = local_call(
        total_body, [shaped((near, cols), F32), shaped((rank, rank), F32)], exchange(pieces, "mp")
    )
    q_row = jnp.sum(exchange(q_part, CHIPS), axis=0) / replicas
    mixed = sent_to_all(q_row, DP)

    (inverse,) = local_call(inverse_body, [shaped((rank, rank), F32)], gram, flops=4 * rank**3)
    p_hat = nn(inverse, p_t, precision=HIGHEST)
    q_own, q_copies = local_call(
        own_body,
        [shaped((rank, cols), F32), shaped((shards, rank, cols), BF16)],
        inverse,
        mixed,
        flops=12 * rank * rank * cols,
    )

    q_parts = exchange(q_copies, "mp")
    new_error = residue(q_parts, p_hat.astype(BF16).T, merged)
    scale = jnp.sqrt(F32(rows * shards))
    return (new_error, (p_hat * scale).T, q_own.T)


def solution(mesh):
    finer = Mesh(mesh.devices.reshape(4, 8, 2, mesh.shape["mp"]), ("dp_0", "dp_1", "dp_2", "mp"))
    in_specs = (P(DP, "mp"), P(DP, "mp"), P(DP_MP, None), P("mp", None))
    out_specs = (P(DP_MP, None), P("mp", None), P("mp", None))
    return jax.shard_map(layer, mesh=finer, in_specs=in_specs, out_specs=out_specs, check_vma=False)
```

```python
import functools

import jax
import jax.numpy as jnp
from jax import lax
from jax.experimental import pallas as pl
from jax.experimental.pallas import tpu as pltpu
from jax.sharding import Mesh
from jax.sharding import PartitionSpec as P

DP = ("dp_0", "dp_1", "dp_2")
DP_MP = ("dp_0", "dp_1", "dp_2", "mp")
BF16 = jnp.bfloat16
F32 = jnp.float32
HIGHEST = lax.Precision.HIGHEST
GRANT = 16 * 1024 * 1024
WIDE_GRANT = 50 * 1024 * 1024


def exchange(pieces, axes):
    return lax.all_to_all(pieces, axes, split_axis=0, concat_axis=0, tiled=True)


def sent_to_all(shard, axes):
    return exchange(jnp.broadcast_to(shard, (lax.axis_size(axes), *shard.shape)), axes)


def nt(a, b, **kw):
    return lax.dot_general(a, b, (((1,), (1,)), ((), ())), preferred_element_type=F32, **kw)


def nn(a, b, **kw):
    return lax.dot_general(a, b, (((1,), (0,)), ((), ())), preferred_element_type=F32, **kw)


def local_call(body, outs, *args, flops=0):
    spec = pl.BlockSpec(memory_space=pltpu.VMEM)
    moved = sum(a.size * a.dtype.itemsize for a in (*args, *outs))
    return pl.pallas_call(
        body,
        out_shape=list(outs),
        in_specs=[spec] * len(args),
        out_specs=[spec] * len(outs),
        compiler_params=pltpu.CompilerParams(vmem_limit_bytes=GRANT),
        cost_estimate=pl.CostEstimate(flops=flops, bytes_accessed=moved, transcendentals=0),
    )(*args)


def shaped(shape, dtype):
    return jax.ShapeDtypeStruct(shape, dtype)


def start_body(x_ref, q_ref, out_ref):
    tokens = x_ref.shape[1]
    q = q_ref[...]
    high = q.astype(BF16)
    low = (q - high.astype(F32)).astype(BF16)
    x = x_ref[...]
    out_ref[:, :tokens] = (nn(high, x) + nn(low, x)).astype(BF16)
    out_ref[:, tokens:] = high


def p_body(first_ref, g_ref, e_ref, out_ref):
    tokens = g_ref.shape[0]
    shards = first_ref.shape[0]
    xq = first_ref[0, :, :tokens].astype(F32)
    for i in range(1, shards):
        xq = xq + first_ref[i, :, :tokens].astype(F32)
    q_full = jnp.concatenate([first_ref[i, :, tokens:] for i in range(shards)], axis=1)
    out_ref[...] = nn(xq.astype(BF16), g_ref[...]) + nt(q_full, e_ref[...])


def column_tiles(width, tile=512):
    return [(start, min(start + tile, width)) for start in range(0, width, tile)]


def merged_body(g_ref, e_hbm, x_hbm, out_ref, e_ref, x_ref, sems):
    copies = []
    for i, (lo, hi) in enumerate(column_tiles(out_ref.shape[1])):
        pair = (
            pltpu.make_async_copy(x_hbm.at[lo:hi, :], x_ref.at[lo:hi, :], sems.at[0, i]),
            pltpu.make_async_copy(e_hbm.at[:, lo:hi], e_ref.at[:, lo:hi], sems.at[1, i]),
        )
        for copy in pair:
            copy.start()
        copies.append(pair)
    g = g_ref[...]
    for (lo, hi), pair in zip(column_tiles(out_ref.shape[1]), copies):
        for copy in pair:
            copy.wait()
        made = nt(g, x_ref[lo:hi, :]) + e_ref[:, lo:hi].astype(F32)
        out_ref[:, lo:hi] = made.astype(BF16)


def merge(g_t, error, x_full):
    rows, width = error.shape
    return pl.pallas_call(
        merged_body,
        name="merged",
        out_shape=shaped((rows, width), BF16),
        in_specs=[
            pl.BlockSpec(memory_space=pltpu.VMEM),
            pl.BlockSpec(memory_space=pltpu.HBM),
            pl.BlockSpec(memory_space=pltpu.HBM),
        ],
        out_specs=pl.BlockSpec(memory_space=pltpu.VMEM),
        scratch_shapes=[
            pltpu.VMEM(error.shape, error.dtype),
            pltpu.VMEM(x_full.shape, x_full.dtype),
            pltpu.SemaphoreType.DMA((2, len(column_tiles(width)))),
        ],
        compiler_params=pltpu.CompilerParams(vmem_limit_bytes=WIDE_GRANT),
        cost_estimate=pl.CostEstimate(
            flops=2 * rows * width * g_t.shape[1],
            bytes_accessed=4 * rows * width + 2 * x_full.size,
            transcendentals=0,
        ),
    )(g_t, error, x_full)


def product_body(p_ref, merged_ref, out_ref, gram_ref):
    rank = p_ref.shape[0]
    width = merged_ref.shape[1]
    half = out_ref.shape[0]
    p = p_ref[...]
    gram_ref[...] = nt(p, p, precision=HIGHEST)
    p_b = p.astype(BF16)
    for lo, hi in column_tiles(half):
        left = nn(p_b, merged_ref[:, lo:hi])
        end = min(half + hi, width)
        right = nn(p_b, merged_ref[:, half + lo : end])
        spare = half + hi - end
        if spare:
            right = jnp.concatenate([right, jnp.zeros((rank, spare), F32)], axis=1)
        out_ref[lo:hi, :] = jnp.concatenate([left, right], axis=0).T.astype(BF16)


def spread_body(arrived_ref, gram_ref, out_ref):
    shards, size, _ = out_ref.shape
    near = size // 2
    total = arrived_ref[:near, :].astype(F32)
    for i in range(1, arrived_ref.shape[0] // near):
        total = total + arrived_ref[i * near : (i + 1) * near, :].astype(F32)
    rank = gram_ref.shape[0]
    gram = jnp.concatenate([gram_ref[: rank // 2, :], gram_ref[rank // 2 :, :]], axis=1)
    for i in range(shards):
        out_ref[i, :near, :] = total
        out_ref[i, near:, :] = gram


def settle_body(second_ref, out_ref, gram_ref, *, replicas):
    near = second_ref.shape[1] // 2
    rank = gram_ref.shape[0]
    total = second_ref[0]
    for i in range(1, second_ref.shape[0]):
        total = total + second_ref[i]
    gram_ref[: rank // 2, :] = total[near:, :rank]
    gram_ref[rank // 2 :, :] = total[near:, rank:]
    rounded = (total[:near, :] / replicas).astype(BF16)
    for i in range(out_ref.shape[0] // near):
        out_ref[i * near : (i + 1) * near, :] = rounded


def inverse_body(gram_ref, out_ref):
    rank = gram_ref.shape[0]
    row = lax.broadcasted_iota(jnp.int32, (rank, rank), 0)
    col = lax.broadcasted_iota(jnp.int32, (rank, rank), 1)
    eye = (row == col).astype(F32)
    gram = gram_ref[...]
    trace = jnp.sum(jnp.sum(gram * eye, axis=1, keepdims=True), axis=0, keepdims=True)
    ridge = 0.01 * trace / rank + 1e-06
    work = jnp.concatenate([gram + ridge * eye, eye], axis=1)
    below = lax.broadcasted_iota(jnp.int32, (rank, 2 * rank), 0)
    done = []
    for k in range(0, rank, 2):
        first, second = work[k : k + 1, :], work[k + 1 : k + 2, :]
        pivot = jnp.broadcast_to(first[:, k : k + 1], first.shape)
        cross = jnp.broadcast_to(first[:, k + 1 : k + 2], first.shape)
        pivot_2 = jnp.broadcast_to(second[:, k + 1 : k + 2], first.shape)
        left = jnp.broadcast_to(work[:, k : k + 1], work.shape)
        right = jnp.broadcast_to(work[:, k + 1 : k + 2], work.shape)
        root = lax.rsqrt(pivot)
        cross = cross * root
        root_2 = lax.rsqrt(pivot_2 - cross * cross)
        first = first * root
        second = (second - cross * first) * root_2
        done.append(first[:, rank:])
        done.append(second[:, rank:])
        if k + 2 < rank:
            rest = below > k + 1
            left = left * root
            right = (right - cross * left) * root_2
            change = left * first + right * second
            work = jnp.where(rest, work - change, work)
    out_ref[...] = jnp.concatenate(done, axis=0)


def residue_body(
    shard_ref, packed_ref, inverse_ref, p_ref, merged_ref, out_hbm, own_ref, out_ref, sems
):
    rank, cols = own_ref.shape
    half = packed_ref.shape[0]
    width = merged_ref.shape[1]
    inverse = inverse_ref[...]
    high = inverse.astype(BF16)
    low = (inverse - high.astype(F32)).astype(BF16)
    none = jnp.zeros((rank, rank), F32)
    twice = jnp.concatenate(
        [jnp.concatenate([inverse.T, none], axis=1), jnp.concatenate([none, inverse.T], axis=1)],
        axis=0,
    )
    twice_high = twice.astype(BF16)
    twice_low = (twice - twice_high.astype(F32)).astype(BF16)
    p_rows = p_ref[...]
    no_rows = jnp.zeros(p_rows.shape, BF16)
    sides = [
        (0, jnp.concatenate([p_rows, no_rows], axis=1)),
        (half, jnp.concatenate([no_rows, p_rows], axis=1)),
    ]
    copies = []
    for lo, hi in column_tiles(half):
        packed = packed_ref[lo:hi, :]
        q = (nn(packed, twice_high) + nn(packed, twice_low)).astype(BF16)
        for start, rows in sides:
            first, last = start + lo, min(start + hi, width)
            approx = nt(rows, q)[:, : last - first]
            made = merged_ref[:, first:last].astype(F32) - approx
            out_ref[:, first:last] = made.astype(BF16)
            copies.append(
                pltpu.make_async_copy(
                    out_ref.at[:, first:last], out_hbm.at[:, first:last], sems.at[len(copies)]
                )
            )
            copies[-1].start()
    for i in range(width // cols):

        @pl.when(shard_ref[0] == i)
        def _():
            first, last = i * cols, (i + 1) * cols
            parts = []
            if first < half:
                parts.append(packed_ref[first : min(last, half), :rank])
            if last > half:
                parts.append(packed_ref[max(first, half) - half : last - half, rank:])
            mine = parts[0] if len(parts) == 1 else jnp.concatenate(parts, axis=0)
            own_ref[...] = nt(high, mine) + nt(low, mine)

    for copy in copies:
        copy.wait()


def residue(shard, packed, inverse, p_rows, merged, cols):
    rows, width = merged.shape
    spec = pl.BlockSpec(memory_space=pltpu.VMEM)
    return pl.pallas_call(
        residue_body,
        name="residue",
        out_shape=[shaped((rows, width), BF16), shaped((inverse.shape[0], cols), F32)],
        in_specs=[pl.BlockSpec(memory_space=pltpu.SMEM), spec, spec, spec, spec],
        out_specs=[pl.BlockSpec(memory_space=pltpu.HBM), spec],
        scratch_shapes=[
            pltpu.VMEM((rows, width), BF16),
            pltpu.SemaphoreType.DMA((2 * len(column_tiles(packed.shape[0])),)),
        ],
        compiler_params=pltpu.CompilerParams(vmem_limit_bytes=GRANT),
        cost_estimate=pl.CostEstimate(
            flops=2 * rows * width * p_rows.shape[1],
            bytes_accessed=4 * rows * width,
            transcendentals=0,
        ),
    )(shard, packed, inverse, p_rows, merged)


def layer(inputs, grad_out, error, q_prev):
    replicas = lax.axis_size(DP)
    shards = lax.axis_size("mp")
    tokens, cols = inputs.shape
    rows = grad_out.shape[1]
    rank = q_prev.shape[1]
    width = error.shape[1]
    x_t = inputs.T
    x_full = lax.all_gather(x_t, "mp", axis=0, tiled=True)

    (sent,) = local_call(
        start_body,
        [shaped((rank, tokens + cols), BF16)],
        x_t,
        q_prev.T,
        flops=4 * rank * tokens * cols,
    )
    first = lax.all_gather(sent, "mp")
    (p_part,) = local_call(
        p_body,
        [shaped((rank, rows), F32)],
        first,
        grad_out,
        error,
        flops=2 * rank * rows * (tokens + width),
    )
    p_row = jnp.sum(exchange(p_part, DP), axis=0) / replicas
    p_t = sent_to_all(p_row, DP)

    merged = merge(grad_out.T, error, x_full)
    near = -(-width // (2 * replicas * 16)) * 16
    product, gram_part = local_call(
        product_body,
        [shaped((replicas * near, 2 * rank), BF16), shaped((rank, rank), F32)],
        p_t,
        merged,
        flops=2 * rows * width * rank,
    )
    (pieces,) = local_call(
        spread_body, [shaped((shards, 2 * near, 2 * rank), F32)], exchange(product, DP), gram_part
    )
    q_copies, gram = local_call(
        functools.partial(settle_body, replicas=replicas),
        [shaped(product.shape, BF16), shaped((rank, rank), F32)],
        exchange(pieces, "mp"),
    )
    packed = exchange(q_copies, DP)
    (inverse,) = local_call(inverse_body, [shaped((rank, rank), F32)], gram, flops=4 * rank**3)
    p_hat = nn(inverse, p_t, precision=HIGHEST)
    shard = lax.axis_index("mp").astype(jnp.int32).reshape(1)
    new_error, q_own = residue(shard, packed, inverse, p_hat.astype(BF16).T, merged, cols)
    scale = jnp.sqrt(F32(rows * shards))
    return (new_error, (p_hat * scale).T, q_own.T)


def solution(mesh):
    finer = Mesh(mesh.devices.reshape(4, 8, 2, mesh.shape["mp"]), ("dp_0", "dp_1", "dp_2", "mp"))
    in_specs = (P(DP, "mp"), P(DP, "mp"), P(DP_MP, None), P("mp", None))
    out_specs = (P(DP_MP, None), P("mp", None), P("mp", None))
    return jax.shard_map(layer, mesh=finer, in_specs=in_specs, out_specs=out_specs, check_vma=False)
```

```python
import functools

import jax
import jax.numpy as jnp
from jax import lax
from jax.experimental import pallas as pl
from jax.experimental.pallas import tpu as pltpu
from jax.sharding import Mesh
from jax.sharding import PartitionSpec as P

DP = ("dp_0", "dp_1", "dp_2")
DP_MP = ("dp_0", "dp_1", "dp_2", "mp")
BF16 = jnp.bfloat16
F32 = jnp.float32
HIGHEST = lax.Precision.HIGHEST
GRANT = 16 * 1024 * 1024
WIDE_GRANT = 50 * 1024 * 1024
START_GRANT = 55000 * 1024


def exchange(pieces, axes):
    return lax.all_to_all(pieces, axes, split_axis=0, concat_axis=0, tiled=True)


def sent_to_all(shard, axes):
    return exchange(jnp.broadcast_to(shard, (lax.axis_size(axes), *shard.shape)), axes)


def nt(a, b, **kw):
    return lax.dot_general(a, b, (((1,), (1,)), ((), ())), preferred_element_type=F32, **kw)


def nn(a, b, **kw):
    return lax.dot_general(a, b, (((1,), (0,)), ((), ())), preferred_element_type=F32, **kw)


def local_call(body, outs, *args, flops=0):
    spec = pl.BlockSpec(memory_space=pltpu.VMEM)
    moved = sum(a.size * a.dtype.itemsize for a in (*args, *outs))
    return pl.pallas_call(
        body,
        out_shape=list(outs),
        in_specs=[spec] * len(args),
        out_specs=[spec] * len(outs),
        compiler_params=pltpu.CompilerParams(vmem_limit_bytes=GRANT),
        cost_estimate=pl.CostEstimate(flops=flops, bytes_accessed=moved, transcendentals=0),
    )(*args)


def shaped(shape, dtype):
    return jax.ShapeDtypeStruct(shape, dtype)


def start_body(x_hbm, q_hbm, out_ref, x_ref, q_ref, sems):
    tokens = x_ref.shape[1]
    x_copy = pltpu.make_async_copy(x_hbm, x_ref, sems.at[0])
    q_copy = pltpu.make_async_copy(q_hbm, q_ref, sems.at[1])
    x_copy.start()
    q_copy.start()
    q_copy.wait()
    q = q_ref[...]
    high = q.astype(BF16)
    low = (q - high.astype(F32)).astype(BF16)
    out_ref[:, tokens:] = high
    x_copy.wait()
    x = x_ref[...]
    out_ref[:, :tokens] = (nn(high, x) + nn(low, x)).astype(BF16)


def started(x_t, q_t):
    cols, tokens = x_t.shape
    rank = q_t.shape[0]
    return pl.pallas_call(
        start_body,
        name="start",
        out_shape=shaped((rank, tokens + cols), BF16),
        in_specs=[pl.BlockSpec(memory_space=pltpu.HBM)] * 2,
        out_specs=pl.BlockSpec(memory_space=pltpu.VMEM),
        scratch_shapes=[
            pltpu.VMEM(x_t.shape, x_t.dtype),
            pltpu.VMEM(q_t.shape, q_t.dtype),
            pltpu.SemaphoreType.DMA((2,)),
        ],
        compiler_params=pltpu.CompilerParams(vmem_limit_bytes=START_GRANT),
        cost_estimate=pl.CostEstimate(
            flops=4 * rank * tokens * cols, bytes_accessed=2 * tokens * cols, transcendentals=0
        ),
    )(x_t, q_t)


def p_body(first_ref, g_ref, e_ref, out_ref):
    tokens = g_ref.shape[0]
    shards = first_ref.shape[0]
    xq = first_ref[0, :, :tokens].astype(F32)
    for i in range(1, shards):
        xq = xq + first_ref[i, :, :tokens].astype(F32)
    q_full = jnp.concatenate([first_ref[i, :, tokens:] for i in range(shards)], axis=1)
    out_ref[...] = nn(xq.astype(BF16), g_ref[...]) + nt(q_full, e_ref[...])


def column_tiles(width, tile=512):
    return [(start, min(start + tile, width)) for start in range(0, width, tile)]


def merged_body(g_ref, e_hbm, x_hbm, out_ref, e_ref, x_ref, sems):
    copies = []
    for i, (lo, hi) in enumerate(column_tiles(out_ref.shape[1])):
        pair = (
            pltpu.make_async_copy(x_hbm.at[lo:hi, :], x_ref.at[lo:hi, :], sems.at[0, i]),
            pltpu.make_async_copy(e_hbm.at[:, lo:hi], e_ref.at[:, lo:hi], sems.at[1, i]),
        )
        for copy in pair:
            copy.start()
        copies.append(pair)
    g = g_ref[...]
    for (lo, hi), pair in zip(column_tiles(out_ref.shape[1]), copies):
        for copy in pair:
            copy.wait()
        made = nt(g, x_ref[lo:hi, :]) + e_ref[:, lo:hi].astype(F32)
        out_ref[:, lo:hi] = made.astype(BF16)


def merge(g_t, error, x_full):
    rows, width = error.shape
    return pl.pallas_call(
        merged_body,
        name="merged",
        out_shape=shaped((rows, width), BF16),
        in_specs=[
            pl.BlockSpec(memory_space=pltpu.VMEM),
            pl.BlockSpec(memory_space=pltpu.HBM),
            pl.BlockSpec(memory_space=pltpu.HBM),
        ],
        out_specs=pl.BlockSpec(memory_space=pltpu.VMEM),
        scratch_shapes=[
            pltpu.VMEM(error.shape, error.dtype),
            pltpu.VMEM(x_full.shape, x_full.dtype),
            pltpu.SemaphoreType.DMA((2, len(column_tiles(width)))),
        ],
        compiler_params=pltpu.CompilerParams(vmem_limit_bytes=WIDE_GRANT),
        cost_estimate=pl.CostEstimate(
            flops=2 * rows * width * g_t.shape[1],
            bytes_accessed=4 * rows * width + 2 * x_full.size,
            transcendentals=0,
        ),
    )(g_t, error, x_full)


def product_body(p_ref, merged_ref, out_ref, gram_ref):
    rank = p_ref.shape[0]
    width = merged_ref.shape[1]
    half = out_ref.shape[0]
    p = p_ref[...]
    gram_ref[...] = nt(p, p, precision=HIGHEST)
    p_b = p.astype(BF16)
    for lo, hi in column_tiles(half):
        left = nn(p_b, merged_ref[:, lo:hi])
        end = min(half + hi, width)
        right = nn(p_b, merged_ref[:, half + lo : end])
        spare = half + hi - end
        if spare:
            right = jnp.concatenate([right, jnp.zeros((rank, spare), F32)], axis=1)
        out_ref[lo:hi, :] = jnp.concatenate([left, right], axis=0).T.astype(BF16)


def spread_body(arrived_ref, gram_ref, out_ref):
    shards, size, _ = out_ref.shape
    rank = gram_ref.shape[0]
    near = size - rank
    total = arrived_ref[:near, :].astype(F32)
    for i in range(1, arrived_ref.shape[0] // near):
        total = total + arrived_ref[i * near : (i + 1) * near, :].astype(F32)
    gram = jnp.concatenate([gram_ref[: rank // 2, :], gram_ref[rank // 2 :, :]], axis=1)
    high = gram.astype(BF16)
    low = (gram - high.astype(F32)).astype(BF16)
    block = jnp.concatenate([high, low, total.astype(BF16)], axis=0)
    for i in range(shards):
        out_ref[i] = block


def settle_body(second_ref, out_ref, gram_ref, *, replicas):
    rank = gram_ref.shape[0]
    near = second_ref.shape[1] - rank
    half = rank // 2
    total = second_ref[0].astype(F32)
    for i in range(1, second_ref.shape[0]):
        total = total + second_ref[i].astype(F32)
    gram = total[:half, :] + total[half:rank, :]
    gram_ref[:half, :] = gram[:, :rank]
    gram_ref[half:, :] = gram[:, rank:]
    rounded = (total[rank:, :] / replicas).astype(BF16)
    for i in range(out_ref.shape[0] // near):
        out_ref[i * near : (i + 1) * near, :] = rounded


def inverse_body(gram_ref, out_ref):
    rank = gram_ref.shape[0]
    row = lax.broadcasted_iota(jnp.int32, (rank, rank), 0)
    col = lax.broadcasted_iota(jnp.int32, (rank, rank), 1)
    eye = (row == col).astype(F32)
    gram = gram_ref[...]
    trace = jnp.sum(jnp.sum(gram * eye, axis=1, keepdims=True), axis=0, keepdims=True)
    ridge = 0.01 * trace / rank + 1e-06
    work = jnp.concatenate([gram + ridge * eye, eye], axis=1)
    below = lax.broadcasted_iota(jnp.int32, (rank, 2 * rank), 0)
    done = []
    for k in range(0, rank, 2):
        first, second = work[k : k + 1, :], work[k + 1 : k + 2, :]
        pivot = jnp.broadcast_to(first[:, k : k + 1], first.shape)
        cross = jnp.broadcast_to(first[:, k + 1 : k + 2], first.shape)
        pivot_2 = jnp.broadcast_to(second[:, k + 1 : k + 2], first.shape)
        left = jnp.broadcast_to(work[:, k : k + 1], work.shape)
        right = jnp.broadcast_to(work[:, k + 1 : k + 2], work.shape)
        root = lax.rsqrt(pivot)
        cross = cross * root
        root_2 = lax.rsqrt(pivot_2 - cross * cross)
        first = first * root
        second = (second - cross * first) * root_2
        done.append(first[:, rank:])
        done.append(second[:, rank:])
        if k + 2 < rank:
            rest = below > k + 1
            left = left * root
            right = (right - cross * left) * root_2
            change = left * first + right * second
            work = jnp.where(rest, work - change, work)
    out_ref[...] = jnp.concatenate(done, axis=0)


def residue_body(
    shard_ref, packed_ref, inverse_ref, p_ref, merged_ref, out_hbm, own_ref, out_ref, sems
):
    rank, cols = own_ref.shape
    half = packed_ref.shape[0]
    width = merged_ref.shape[1]
    inverse = inverse_ref[...]
    high = inverse.astype(BF16)
    low = (inverse - high.astype(F32)).astype(BF16)
    none = jnp.zeros((rank, rank), F32)
    twice = jnp.concatenate(
        [jnp.concatenate([inverse.T, none], axis=1), jnp.concatenate([none, inverse.T], axis=1)],
        axis=0,
    )
    twice_high = twice.astype(BF16)
    twice_low = (twice - twice_high.astype(F32)).astype(BF16)
    p_rows = p_ref[...]
    no_rows = jnp.zeros(p_rows.shape, BF16)
    sides = [
        (0, jnp.concatenate([p_rows, no_rows], axis=1)),
        (half, jnp.concatenate([no_rows, p_rows], axis=1)),
    ]
    copies = []
    for lo, hi in column_tiles(half):
        packed = packed_ref[lo:hi, :]
        q = (nn(packed, twice_high) + nn(packed, twice_low)).astype(BF16)
        for start, rows in sides:
            first, last = start + lo, min(start + hi, width)
            approx = nt(rows, q)[:, : last - first]
            made = merged_ref[:, first:last].astype(F32) - approx
            out_ref[:, first:last] = made.astype(BF16)
            copies.append(
                pltpu.make_async_copy(
                    out_ref.at[:, first:last], out_hbm.at[:, first:last], sems.at[len(copies)]
                )
            )
            copies[-1].start()
    for i in range(width // cols):

        @pl.when(shard_ref[0] == i)
        def _():
            first, last = i * cols, (i + 1) * cols
            parts = []
            if first < half:
                parts.append(packed_ref[first : min(last, half), :rank])
            if last > half:
                parts.append(packed_ref[max(first, half) - half : last - half, rank:])
            mine = parts[0] if len(parts) == 1 else jnp.concatenate(parts, axis=0)
            own_ref[...] = nt(high, mine) + nt(low, mine)

    for copy in copies:
        copy.wait()


def residue(shard, packed, inverse, p_rows, merged, cols):
    rows, width = merged.shape
    spec = pl.BlockSpec(memory_space=pltpu.VMEM)
    return pl.pallas_call(
        residue_body,
        name="residue",
        out_shape=[shaped((rows, width), BF16), shaped((inverse.shape[0], cols), F32)],
        in_specs=[pl.BlockSpec(memory_space=pltpu.SMEM), spec, spec, spec, spec],
        out_specs=[pl.BlockSpec(memory_space=pltpu.HBM), spec],
        scratch_shapes=[
            pltpu.VMEM((rows, width), BF16),
            pltpu.SemaphoreType.DMA((2 * len(column_tiles(packed.shape[0])),)),
        ],
        compiler_params=pltpu.CompilerParams(vmem_limit_bytes=GRANT),
        cost_estimate=pl.CostEstimate(
            flops=2 * rows * width * p_rows.shape[1],
            bytes_accessed=4 * rows * width,
            transcendentals=0,
        ),
    )(shard, packed, inverse, p_rows, merged)


def layer(inputs, grad_out, error, q_prev):
    replicas = lax.axis_size(DP)
    shards = lax.axis_size("mp")
    tokens, cols = inputs.shape
    rows = grad_out.shape[1]
    rank = q_prev.shape[1]
    width = error.shape[1]
    x_t = inputs.T
    x_full = lax.all_gather(x_t, "mp", axis=0, tiled=True)

    sent = started(x_t, q_prev.T)
    first = lax.all_gather(sent, "mp")
    (p_part,) = local_call(
        p_body,
        [shaped((rank, rows), F32)],
        first,
        grad_out,
        error,
        flops=2 * rank * rows * (tokens + width),
    )
    p_row = jnp.sum(exchange(p_part, DP), axis=0) / replicas
    p_t = sent_to_all(p_row, DP)

    merged = merge(grad_out.T, error, x_full)
    near = -(-width // (2 * replicas * 16)) * 16
    product, gram_part = local_call(
        product_body,
        [shaped((replicas * near, 2 * rank), BF16), shaped((rank, rank), F32)],
        p_t,
        merged,
        flops=2 * rows * width * rank,
    )
    (pieces,) = local_call(
        spread_body,
        [shaped((shards, rank + near, 2 * rank), BF16)],
        exchange(product, DP),
        gram_part,
    )
    q_copies, gram = local_call(
        functools.partial(settle_body, replicas=replicas),
        [shaped(product.shape, BF16), shaped((rank, rank), F32)],
        exchange(pieces, "mp"),
    )
    packed = exchange(q_copies, DP)
    (inverse,) = local_call(inverse_body, [shaped((rank, rank), F32)], gram, flops=4 * rank**3)
    p_hat = nn(inverse, p_t, precision=HIGHEST)
    shard = lax.axis_index("mp").astype(jnp.int32).reshape(1)
    new_error, q_own = residue(shard, packed, inverse, p_hat.astype(BF16).T, merged, cols)
    scale = jnp.sqrt(F32(rows * shards))
    return (new_error, (p_hat * scale).T, q_own.T)


def solution(mesh):
    finer = Mesh(mesh.devices.reshape(4, 8, 2, mesh.shape["mp"]), ("dp_0", "dp_1", "dp_2", "mp"))
    in_specs = (P(DP, "mp"), P(DP, "mp"), P(DP_MP, None), P("mp", None))
    out_specs = (P(DP_MP, None), P("mp", None), P("mp", None))
    return jax.shard_map(layer, mesh=finer, in_specs=in_specs, out_specs=out_specs, check_vma=False)
```

```python
import functools

import jax
import jax.numpy as jnp
from jax import lax
from jax.experimental import pallas as pl
from jax.experimental.pallas import tpu as pltpu
from jax.sharding import Mesh
from jax.sharding import PartitionSpec as P

DP = ("dp_0", "dp_1", "dp_2")
CHIPS = ("dp_0", "dp_1")
CORE = "dp_2"
DP_MP = ("dp_0", "dp_1", "dp_2", "mp")
BF16 = jnp.bfloat16
F32 = jnp.float32
HIGHEST = lax.Precision.HIGHEST
GRANT = 16 * 1024 * 1024
WIDE_GRANT = 50 * 1024 * 1024
START_GRANT = 55000 * 1024


def exchange(pieces, axes):
    return lax.all_to_all(pieces, axes, split_axis=0, concat_axis=0, tiled=True)


def sent_to_all(shard, axes):
    return exchange(jnp.broadcast_to(shard, (lax.axis_size(axes), *shard.shape)), axes)


def nt(a, b, **kw):
    return lax.dot_general(a, b, (((1,), (1,)), ((), ())), preferred_element_type=F32, **kw)


def nn(a, b, **kw):
    return lax.dot_general(a, b, (((1,), (0,)), ((), ())), preferred_element_type=F32, **kw)


def local_call(body, outs, *args, flops=0):
    spec = pl.BlockSpec(memory_space=pltpu.VMEM)
    moved = sum(a.size * a.dtype.itemsize for a in (*args, *outs))
    return pl.pallas_call(
        body,
        out_shape=list(outs),
        in_specs=[spec] * len(args),
        out_specs=[spec] * len(outs),
        compiler_params=pltpu.CompilerParams(vmem_limit_bytes=GRANT),
        cost_estimate=pl.CostEstimate(flops=flops, bytes_accessed=moved, transcendentals=0),
    )(*args)


def shaped(shape, dtype):
    return jax.ShapeDtypeStruct(shape, dtype)


def start_body(x_hbm, q_hbm, out_ref, x_ref, q_ref, sems):
    tokens = x_ref.shape[1]
    x_copy = pltpu.make_async_copy(x_hbm, x_ref, sems.at[0])
    q_copy = pltpu.make_async_copy(q_hbm, q_ref, sems.at[1])
    x_copy.start()
    q_copy.start()
    q_copy.wait()
    q = q_ref[...]
    high = q.astype(BF16)
    low = (q - high.astype(F32)).astype(BF16)
    out_ref[:, tokens:] = high
    x_copy.wait()
    x = x_ref[...]
    out_ref[:, :tokens] = (nn(high, x) + nn(low, x)).astype(BF16)


def started(x_t, q_t):
    cols, tokens = x_t.shape
    rank = q_t.shape[0]
    return pl.pallas_call(
        start_body,
        name="start",
        out_shape=shaped((rank, tokens + cols), BF16),
        in_specs=[pl.BlockSpec(memory_space=pltpu.HBM)] * 2,
        out_specs=pl.BlockSpec(memory_space=pltpu.VMEM),
        scratch_shapes=[
            pltpu.VMEM(x_t.shape, x_t.dtype),
            pltpu.VMEM(q_t.shape, q_t.dtype),
            pltpu.SemaphoreType.DMA((2,)),
        ],
        compiler_params=pltpu.CompilerParams(vmem_limit_bytes=START_GRANT),
        cost_estimate=pl.CostEstimate(
            flops=4 * rank * tokens * cols, bytes_accessed=2 * tokens * cols, transcendentals=0
        ),
    )(x_t, q_t)


def p_body(first_ref, g_ref, e_ref, out_ref):
    tokens = g_ref.shape[0]
    shards = first_ref.shape[0]
    xq = first_ref[0, :, :tokens].astype(F32)
    for i in range(1, shards):
        xq = xq + first_ref[i, :, :tokens].astype(F32)
    q_full = jnp.concatenate([first_ref[i, :, tokens:] for i in range(shards)], axis=1)
    out_ref[...] = nn(xq.astype(BF16), g_ref[...]) + nt(q_full, e_ref[...])


def column_tiles(width, tile=512):
    return [(start, min(start + tile, width)) for start in range(0, width, tile)]


def merged_body(g_ref, e_hbm, x_hbm, out_ref, e_ref, x_ref, sems):
    copies = []
    for i, (lo, hi) in enumerate(column_tiles(out_ref.shape[1])):
        pair = (
            pltpu.make_async_copy(x_hbm.at[lo:hi, :], x_ref.at[lo:hi, :], sems.at[0, i]),
            pltpu.make_async_copy(e_hbm.at[:, lo:hi], e_ref.at[:, lo:hi], sems.at[1, i]),
        )
        for copy in pair:
            copy.start()
        copies.append(pair)
    g = g_ref[...]
    for (lo, hi), pair in zip(column_tiles(out_ref.shape[1]), copies):
        for copy in pair:
            copy.wait()
        made = nt(g, x_ref[lo:hi, :]) + e_ref[:, lo:hi].astype(F32)
        out_ref[:, lo:hi] = made.astype(BF16)


def merge(g_t, error, x_full):
    rows, width = error.shape
    return pl.pallas_call(
        merged_body,
        name="merged",
        out_shape=shaped((rows, width), BF16),
        in_specs=[
            pl.BlockSpec(memory_space=pltpu.VMEM),
            pl.BlockSpec(memory_space=pltpu.HBM),
            pl.BlockSpec(memory_space=pltpu.HBM),
        ],
        out_specs=pl.BlockSpec(memory_space=pltpu.VMEM),
        scratch_shapes=[
            pltpu.VMEM(error.shape, error.dtype),
            pltpu.VMEM(x_full.shape, x_full.dtype),
            pltpu.SemaphoreType.DMA((2, len(column_tiles(width)))),
        ],
        compiler_params=pltpu.CompilerParams(vmem_limit_bytes=WIDE_GRANT),
        cost_estimate=pl.CostEstimate(
            flops=2 * rows * width * g_t.shape[1],
            bytes_accessed=4 * rows * width + 2 * x_full.size,
            transcendentals=0,
        ),
    )(g_t, error, x_full)


def product_body(p_ref, merged_ref, out_ref, gram_ref):
    rank = p_ref.shape[0]
    width = merged_ref.shape[1]
    half = out_ref.shape[0]
    p = p_ref[...]
    gram_ref[...] = nt(p, p, precision=HIGHEST)
    p_b = p.astype(BF16)
    for lo, hi in column_tiles(half):
        left = nn(p_b, merged_ref[:, lo:hi])
        end = min(half + hi, width)
        right = nn(p_b, merged_ref[:, half + lo : end])
        spare = half + hi - end
        if spare:
            right = jnp.concatenate([right, jnp.zeros((rank, spare), F32)], axis=1)
        out_ref[lo:hi, :] = jnp.concatenate([left, right], axis=0).T


def pair_body(arrived_ref, out_ref):
    near = out_ref.shape[0]
    out_ref[...] = (arrived_ref[:near, :] + arrived_ref[near:, :]).astype(BF16)


def spread_body(arrived_ref, gram_ref, out_ref):
    shards, size, _ = out_ref.shape
    rank = gram_ref.shape[0]
    near = size - rank
    total = arrived_ref[:near, :].astype(F32)
    for i in range(1, arrived_ref.shape[0] // near):
        total = total + arrived_ref[i * near : (i + 1) * near, :].astype(F32)
    gram = jnp.concatenate([gram_ref[: rank // 2, :], gram_ref[rank // 2 :, :]], axis=1)
    high = gram.astype(BF16)
    low = (gram - high.astype(F32)).astype(BF16)
    block = jnp.concatenate([high, low, total.astype(BF16)], axis=0)
    for i in range(shards):
        out_ref[i] = block


def settle_body(second_ref, out_ref, gram_ref, *, replicas):
    rank = gram_ref.shape[0]
    near = second_ref.shape[1] - rank
    half = rank // 2
    total = second_ref[0].astype(F32)
    for i in range(1, second_ref.shape[0]):
        total = total + second_ref[i].astype(F32)
    gram = total[:half, :] + total[half:rank, :]
    gram_ref[:half, :] = gram[:, :rank]
    gram_ref[half:, :] = gram[:, rank:]
    rounded = (total[rank:, :] / replicas).astype(BF16)
    for i in range(out_ref.shape[0] // near):
        out_ref[i * near : (i + 1) * near, :] = rounded


def inverse_body(gram_ref, out_ref):
    rank = gram_ref.shape[0]
    row = lax.broadcasted_iota(jnp.int32, (rank, rank), 0)
    col = lax.broadcasted_iota(jnp.int32, (rank, rank), 1)
    eye = (row == col).astype(F32)
    gram = gram_ref[...]
    trace = jnp.sum(jnp.sum(gram * eye, axis=1, keepdims=True), axis=0, keepdims=True)
    ridge = 0.01 * trace / rank + 1e-06
    work = jnp.concatenate([gram + ridge * eye, eye], axis=1)
    below = lax.broadcasted_iota(jnp.int32, (rank, 2 * rank), 0)
    done = []
    for k in range(0, rank, 2):
        first, second = work[k : k + 1, :], work[k + 1 : k + 2, :]
        pivot = jnp.broadcast_to(first[:, k : k + 1], first.shape)
        cross = jnp.broadcast_to(first[:, k + 1 : k + 2], first.shape)
        pivot_2 = jnp.broadcast_to(second[:, k + 1 : k + 2], first.shape)
        left = jnp.broadcast_to(work[:, k : k + 1], work.shape)
        right = jnp.broadcast_to(work[:, k + 1 : k + 2], work.shape)
        root = lax.rsqrt(pivot)
        cross = cross * root
        root_2 = lax.rsqrt(pivot_2 - cross * cross)
        first = first * root
        second = (second - cross * first) * root_2
        done.append(first[:, rank:])
        done.append(second[:, rank:])
        if k + 2 < rank:
            rest = below > k + 1
            left = left * root
            right = (right - cross * left) * root_2
            change = left * first + right * second
            work = jnp.where(rest, work - change, work)
    out_ref[...] = jnp.concatenate(done, axis=0)


def residue_body(
    shard_ref, packed_ref, inverse_ref, p_ref, merged_ref, out_hbm, own_ref, out_ref, sems
):
    rank, cols = own_ref.shape
    half = packed_ref.shape[0]
    width = merged_ref.shape[1]
    inverse = inverse_ref[...]
    high = inverse.astype(BF16)
    low = (inverse - high.astype(F32)).astype(BF16)
    none = jnp.zeros((rank, rank), F32)
    twice = jnp.concatenate(
        [jnp.concatenate([inverse.T, none], axis=1), jnp.concatenate([none, inverse.T], axis=1)],
        axis=0,
    )
    twice_high = twice.astype(BF16)
    twice_low = (twice - twice_high.astype(F32)).astype(BF16)
    p_rows = p_ref[...]
    no_rows = jnp.zeros(p_rows.shape, BF16)
    sides = [
        (0, jnp.concatenate([p_rows, no_rows], axis=1)),
        (half, jnp.concatenate([no_rows, p_rows], axis=1)),
    ]
    copies = []
    for lo, hi in column_tiles(half, 1024):
        packed = packed_ref[lo:hi, :]
        q = (nn(packed, twice_high) + nn(packed, twice_low)).astype(BF16)
        for start, rows in sides:
            first, last = start + lo, min(start + hi, width)
            approx = nt(rows, q)[:, : last - first]
            made = merged_ref[:, first:last].astype(F32) - approx
            out_ref[:, first:last] = made.astype(BF16)
            copies.append(
                pltpu.make_async_copy(
                    out_ref.at[:, first:last], out_hbm.at[:, first:last], sems.at[len(copies)]
                )
            )
            copies[-1].start()
    for i in range(width // cols):

        @pl.when(shard_ref[0] == i)
        def _():
            first, last = i * cols, (i + 1) * cols
            parts = []
            if first < half:
                parts.append(packed_ref[first : min(last, half), :rank])
            if last > half:
                parts.append(packed_ref[max(first, half) - half : last - half, rank:])
            mine = parts[0] if len(parts) == 1 else jnp.concatenate(parts, axis=0)
            own_ref[...] = nt(high, mine) + nt(low, mine)

    for copy in copies:
        copy.wait()


def residue(shard, packed, inverse, p_rows, merged, cols):
    rows, width = merged.shape
    spec = pl.BlockSpec(memory_space=pltpu.VMEM)
    return pl.pallas_call(
        residue_body,
        name="residue",
        out_shape=[shaped((rows, width), BF16), shaped((inverse.shape[0], cols), F32)],
        in_specs=[pl.BlockSpec(memory_space=pltpu.SMEM), spec, spec, spec, spec],
        out_specs=[pl.BlockSpec(memory_space=pltpu.HBM), spec],
        scratch_shapes=[
            pltpu.VMEM((rows, width), BF16),
            pltpu.SemaphoreType.DMA((2 * len(column_tiles(packed.shape[0], 1024)),)),
        ],
        compiler_params=pltpu.CompilerParams(vmem_limit_bytes=GRANT),
        cost_estimate=pl.CostEstimate(
            flops=2 * rows * width * p_rows.shape[1],
            bytes_accessed=4 * rows * width,
            transcendentals=0,
        ),
    )(shard, packed, inverse, p_rows, merged)


def layer(inputs, grad_out, error, q_prev):
    replicas = lax.axis_size(DP)
    shards = lax.axis_size("mp")
    tokens, cols = inputs.shape
    rows = grad_out.shape[1]
    rank = q_prev.shape[1]
    width = error.shape[1]
    x_t = inputs.T
    x_full = lax.all_gather(x_t, "mp", axis=0, tiled=True)

    sent = started(x_t, q_prev.T)
    first = lax.all_gather(sent, "mp")
    (p_part,) = local_call(
        p_body,
        [shaped((rank, rows), F32)],
        first,
        grad_out,
        error,
        flops=2 * rank * rows * (tokens + width),
    )
    p_row = jnp.sum(exchange(p_part, DP), axis=0) / replicas
    p_t = sent_to_all(p_row, DP)

    merged = merge(grad_out.T, error, x_full)
    near = -(-width // (2 * replicas * 16)) * 16
    product, gram_part = local_call(
        product_body,
        [shaped((replicas * near, 2 * rank), F32), shaped((rank, rank), F32)],
        p_t,
        merged,
        flops=2 * rows * width * rank,
    )
    own = replicas * near // lax.axis_size(CORE)
    (summed,) = local_call(pair_body, [shaped((own, 2 * rank), BF16)], exchange(product, CORE))
    (pieces,) = local_call(
        spread_body,
        [shaped((shards, rank + near, 2 * rank), BF16)],
        exchange(summed, CHIPS),
        gram_part,
    )
    q_copies, gram = local_call(
        functools.partial(settle_body, replicas=replicas),
        [shaped(summed.shape, BF16), shaped((rank, rank), F32)],
        exchange(pieces, "mp"),
    )
    packed = sent_to_all(exchange(q_copies, CHIPS), CORE).reshape(product.shape)
    (inverse,) = local_call(inverse_body, [shaped((rank, rank), F32)], gram, flops=4 * rank**3)
    p_hat = nn(inverse, p_t, precision=HIGHEST)
    shard = lax.axis_index("mp").astype(jnp.int32).reshape(1)
    new_error, q_own = residue(shard, packed, inverse, p_hat.astype(BF16).T, merged, cols)
    scale = jnp.sqrt(F32(rows * shards))
    return (new_error, (p_hat * scale).T, q_own.T)


def solution(mesh):
    finer = Mesh(mesh.devices.reshape(4, 8, 2, mesh.shape["mp"]), ("dp_0", "dp_1", "dp_2", "mp"))
    in_specs = (P(DP, "mp"), P(DP, "mp"), P(DP_MP, None), P("mp", None))
    out_specs = (P(DP_MP, None), P("mp", None), P("mp", None))
    return jax.shard_map(layer, mesh=finer, in_specs=in_specs, out_specs=out_specs, check_vma=False)
```
